128 devices in a mesh: rows: 32 (over z, y, core), cols: 4 (over x).
Axes of the slice: x: 4, y: 4, z: 4, core: 2. Of those that a mesh axis runs over, the one named last changes fastest.
Arguments:
- w_gate: float32 [2048, 8192], P('rows', 'cols'), may hold values from -0.25 to 0.25
- first_gate: float32 [2048, 8192], P('rows', 'cols'), may hold values from -6 to 6
- second_gate: float32 [2048, 8192], P('rows', 'cols'), may hold values from 0.1 to 10
- w_up: float32 [2048, 8192], P('rows', 'cols'), may hold values from -0.25 to 0.25
- first_up: float32 [2048, 8192], P('rows', 'cols'), may hold values from -6 to 6
- second_up: float32 [2048, 8192], P('rows', 'cols'), may hold values from 0.1 to 10
- norm_train: float32 [2048], P(('rows', 'cols')), may hold values from 0.25 to 1.75
- norm_step: float32 [2048], P(('rows', 'cols')), may hold values from -0.3 to 0.3
Outputs:
- ready_gate: bfloat16 [2048, 8192], P(None, 'cols')
- ready_up: bfloat16 [2048, 8192], P(None, 'cols')
- column_gate: float32 [8192], P('cols')
- column_up: float32 [8192], P('cols')
- serve_norm: bfloat16 [2048], replicated
- latest_gate: float32 [2048, 8192], P('rows', 'cols')
- latest_up: float32 [2048, 8192], P('rows', 'cols')
The draws below stay inside these ranges and needn't reach their ends.
All inputs are finite; a program needn't handle non-finite values. Where the reference program divides by a largest or mean magnitude, that divisor is 1e-20 or more.
Results may differ from the reference program's by a relative error of at most 0.001.
Values may be sent and summed in bfloat16 or wider, within the bound.
A program may use at most 128 MiB of HBM per device.

```python
import math
import jax
import jax.numpy as jnp
from jax import lax

D_MODEL = 2048
D_INNER = 8192


def raised(result, key, source, target, parts, factor):
    def block_of(axis_at):
        return (jnp.arange(result.shape[axis_at]) // (result.shape[axis_at] // parts)).reshape((-1,) + (1,) * (result.ndim - 1 - axis_at))

    one_side = jax.random.permutation(key, parts)[block_of(target)]
    other_side = (block_of(target) + parts // 2) % parts
    return jnp.where((block_of(source) == one_side) | (block_of(source) == other_side), factor * result, result)


def levels(key, extent, shards, low, top_value):
    factor_of, own = 1.0, jax.random.fold_in(key, 6)
    for position, shards_of in shards:
        heights = jnp.exp(jax.random.uniform(jax.random.fold_in(own, position), (shards_of,), jnp.float32, low / len(shards), top_value / len(shards)))
        factor_of = factor_of * jnp.repeat(heights, extent[position] // shards_of).reshape([-1 if axis == position else 1 for axis in range(len(extent))])
    return factor_of


def noise(stream_key, dims, scale, bound, cuts=(), held_as=jnp.bfloat16):
    entries = jax.random.normal(stream_key, dims, jnp.float32) * scale
    if len(cuts) > 0:
        entries = levels(stream_key, dims, cuts, -0.22, 0.18) * entries
    return jnp.clip(entries, min=-bound, max=bound).astype(held_as)


def gaussian_with(rng, dims, width, limit, pieces, heavy, kind=jnp.bfloat16):
    entries = width * jax.random.normal(rng, dims, jnp.float32)
    if pieces:
        entries = entries * levels(rng, dims, pieces, -0.22, 0.18)
    return jnp.clip(raised(entries, jax.random.fold_in(rng, 3), *heavy), -limit, limit).astype(kind)


def setup_inputs(seed: int = 0) -> dict:
    streams_of = jax.random.split(jax.random.key(seed), 9)
    w_gate = gaussian_with(streams_of[0], (D_MODEL, D_INNER), D_MODEL ** -0.5, 0.25, ((0, 32), (1, 4)), (0, 1, 32, 2.75), jnp.float32)
    first_gate = noise(streams_of[1], (D_MODEL, D_INNER), 1.0, 6.0, ((0, 32), (1, 4)), jnp.float32)
    second_gate = jnp.clip(jnp.exp(math.log(10.0) - 4.6051702 * jax.random.uniform(streams_of[2], (D_MODEL, D_INNER), jnp.float32) ** levels(streams_of[2], (D_MODEL, D_INNER), ((0, 32), (1, 4)), -0.2, 0.2)), 0.1, 10.0)
    w_up = gaussian_with(streams_of[3], (D_MODEL, D_INNER), D_MODEL ** -0.5, 0.25, ((0, 32), (1, 4)), (0, 1, 32, 2.75), jnp.float32)
    first_up = noise(streams_of[4], (D_MODEL, D_INNER), 1.0, 6.0, ((0, 32), (1, 4)), jnp.float32)
    second_up = jnp.clip(jnp.exp(math.log(10.0) - 4.6051702 * jax.random.uniform(streams_of[5], (D_MODEL, D_INNER), jnp.float32) ** levels(streams_of[5], (D_MODEL, D_INNER), ((0, 32), (1, 4)), -0.2, 0.2)), 0.1, 10.0)
    norm_train = jnp.clip(1.0 + 0.15 * jax.random.normal(streams_of[6], (D_MODEL,), jnp.float32), 0.25, 1.75)
    norm_step = jnp.clip(jax.random.uniform(streams_of[7], (D_MODEL,), jnp.float32, -0.3, 0.3) * levels(streams_of[7], (D_MODEL,), ((0, 128),), -0.4, 0.0), -0.3, 0.3)
    return dict(w_gate=w_gate, first_gate=first_gate, second_gate=second_gate, w_up=w_up, first_up=first_up, second_up=second_up, norm_train=norm_train, norm_step=norm_step)


learn_rate = 0.01
decay_rate = 0.1
tiny_value = 1e-08

def reference(w_gate, first_gate, second_gate, w_up, first_up, second_up, norm_train, norm_step):
    latest_gate = w_gate - learn_rate * (first_gate / (jnp.sqrt(second_gate) + tiny_value) + decay_rate * w_gate)
    latest_up = w_up - learn_rate * (first_up / (jnp.sqrt(second_up) + tiny_value) + decay_rate * w_up)
    column_gate = lax.optimization_barrier(jnp.sum(jnp.abs(latest_gate), axis=0)) / D_MODEL
    ready_gate = (latest_gate / column_gate).astype(jnp.bfloat16)
    column_up = lax.optimization_barrier(jnp.sum(jnp.abs(latest_up), axis=0)) / D_MODEL
    ready_up = (latest_up / column_up).astype(jnp.bfloat16)
    serve_norm = (norm_train + norm_step).astype(jnp.bfloat16)
    return (ready_gate, ready_up, column_gate, column_up, serve_norm, latest_gate, latest_up)
```

```python
import heapq

import jax
import jax.numpy as jnp
from jax import lax
from jax.experimental import pallas as pl
from jax.experimental.pallas import tpu as pltpu
from jax.sharding import PartitionSpec as P

D_MODEL = 2048
WIDTH = 2048
ROWS = 64
SIDE = 4
MESH = pl.DeviceIdType.MESH

learn_rate = 0.01
decay_rate = 0.1
tiny_value = 1e-08

PIECE = 32
CHUNKS = tuple((mat, off) for off in range(0, ROWS, PIECE) for mat in range(2))
LOW = tuple(range(len(CHUNKS) // 2))
HIGH = tuple(range(len(CHUNKS) // 2, len(CHUNKS)))


def follow_ups(da, db, c):
    if (da, db) == (0, 0):
        return ("A+", "A-", "B+", "B-")
    if db == 0:
        on = ("B+", "B-")
        if da == 3 and c in LOW:
            on = ("A+",) + on
        if da == 1 and c in HIGH:
            on = ("A-",) + on
        return on
    if db == 3 and c in LOW:
        return ("B+",)
    if db == 1 and c in HIGH:
        return ("B-",)
    return ()


def seen_by_receiver(link, da, db):
    step = -1 if link[1] == "+" else 1
    return ((da + step) % 4, db) if link[0] == "A" else (da, (db + step) % 4)


def arrival_order():
    unit, delay = 1.0, 1.4 * len(CHUNKS) / 4
    queues = {k: [] for k in ("A+", "A-", "B+", "B-")}
    done = {k: 0.0 for k in queues}
    events = [(0.0, c, (0, 0, c)) for c in range(len(CHUNKS))]
    order, now, serial = [], 0.0, len(CHUNKS)
    while events or any(queues.values()):
        rate = {}
        for k in queues:
            if queues[k]:
                other = ("B" if k[0] == "A" else "A") + k[1]
                rate[k] = (0.5 if queues[other] else 1.0) / unit
        steps = [(1 - done[k]) / rate[k] for k in rate]
        if events:
            steps.append(events[0][0] - now)
        dt = max(0.0, min(steps))
        now += dt
        for k in rate:
            done[k] += rate[k] * dt
            if done[k] >= 1 - 1e-9:
                da, db, c = queues[k].pop(0)
                done[k] = 0.0
                serial += 1
                heapq.heappush(events, (now + delay, serial, seen_by_receiver(k, da, db) + (c,)))
        while events and events[0][0] <= now + 1e-9:
            item = heapq.heappop(events)[2]
            order.append(item)
            for k in follow_ups(*item):
                queues[k].append(item)
    return order


ORDER = arrival_order()


def gather_kernel(
    w_g, f_g, s_g, w_u, f_u, s_u, norm_in,
    out_g, out_u, col_g, col_u, norm_out, latest_g, latest_u,
    first, second, part, pair, inverse, slots, nslots,
    load_sem, send_sem, recv_sem, die_send, die_recv, sum_send, sum_recv, n_send, n_recv,
):
    row = lax.axis_index("rows")
    x = lax.axis_index("cols")
    core = row % 2
    y = (row // 2) % 4
    z = row // 8
    a = y * (1 - core) + z * core
    b = z * (1 - core) + y * core
    stride_a = 2 + 6 * core
    stride_b = 8 - 6 * core
    partner = row + 1 - 2 * core
    outs = (out_g, out_u)

    def at_a(pos):
        return row + ((pos % 4) - a) * stride_a

    def at_b(pos):
        return row + ((pos % 4) - b) * stride_b

    def at_y(pos):
        return row + ((pos % 4) - y) * 2

    def at_z(pos):
        return row + ((pos % 4) - z) * 8

    latest = (latest_g, latest_u)
    loads = []
    for m, (w, f, s) in enumerate(((w_g, f_g, s_g), (w_u, f_u, s_u))):
        for j, (src, dst) in enumerate(((w, latest[m]), (f, first.at[m]), (s, second.at[m]))):
            copy = pltpu.make_async_copy(src, dst, load_sem.at[3 * m + j])
            copy.start()
            loads.append(copy)

    barrier = pltpu.get_barrier_semaphore()
    peers = [(partner, x)]
    for d in range(1, 4):
        peers += [(at_y(y + d), x), (at_z(z + d), x), (row, (x + d) % 4)]
    for peer in peers:
        pl.semaphore_signal(barrier, inc=1, device_id=peer, device_id_type=MESH)

    for m in range(2):
        for copy in loads[3 * m : 3 * m + 3]:
            copy.wait()

        def step(i, acc, m=m):
            at = pl.ds(pl.multiple_of(i * 8, 8), 8)
            w = latest[m][at, :]
            new = w - learn_rate * (
                first[m, at, :] / (jnp.sqrt(second[m, at, :]) + tiny_value) + decay_rate * w
            )
            latest[m][at, :] = new
            return acc + jnp.abs(new)

        acc = lax.fori_loop(0, ROWS // 8, step, jnp.zeros((8, WIDTH), jnp.float32))
        part[m] = jnp.sum(acc, axis=0, keepdims=True)

    pl.semaphore_wait(barrier, len(peers))

    def remote(src, dst, send, recv, device):
        return pltpu.make_async_remote_copy(
            src_ref=src, dst_ref=dst, send_sem=send, recv_sem=recv,
            device_id=device, device_id_type=MESH,
        )

    sent = []

    def start(copy):
        copy.start()
        sent.append(copy)

    both = remote(part, pair, sum_send.at[0], sum_recv.at[0], (partner, x))
    start(both)

    def norm_stage(i, device_of, me):
        mine = nslots.at[i, me]
        for d in range(1, 4):
            start(remote(mine, mine, n_send.at[3 * i + d - 1], n_recv.at[3 * i + d - 1],
                         device_of(d)))

    def norm_wait(i, me):
        total = None
        for d in range(1, 4):
            frm = (me + 4 - d) % 4
            remote(nslots.at[i, frm], nslots.at[i, frm], n_send.at[3 * i + d - 1],
                   n_recv.at[3 * i + d - 1], (partner, x)).wait_recv()
        for k in range(4):
            total = nslots[i, k] if total is None else total + nslots[i, k]
        return total

    device = row * 4 + x
    nslots[0, x] = norm_in[...]
    norm_stage(0, lambda d: (row, (x + d) % 4), x)

    both.wait_recv()
    places = ((y, z), (z, y))
    movers = ((at_y, at_z), (at_z, at_y))
    for m in range(2):
        slots[0, m, places[m][0]] = part[m] + pair[m]
    for stage in range(2):
        for d in range(1, 4):
            for m in range(2):
                me = places[m][stage]
                mine = slots.at[stage, m, me]
                k = 1 + (stage * 2 + m) * 3 + d - 1
                start(remote(mine, mine, sum_send.at[k], sum_recv.at[k],
                             (movers[m][stage](me + d), x)))
        for m in range(2):
            me = places[m][stage]
            for d in range(1, 4):
                frm = (me + 4 - d) % 4
                k = 1 + (stage * 2 + m) * 3 + d - 1
                remote(slots.at[stage, m, frm], slots.at[stage, m, frm], sum_send.at[k],
                       sum_recv.at[k], (partner, x)).wait_recv()
            total = slots[stage, m, 0]
            for k in range(1, 4):
                total = total + slots[stage, m, k]
            if stage == 0:
                slots[1, m, places[m][1]] = total
            else:
                column = total * (1.0 / D_MODEL)
                (col_g, col_u)[m][...] = column
                inverse[m] = 1.0 / column

    def block_row(da, db, of_core=None):
        return row + ((a + da) % 4 - a) * stride_a + ((b + db) % 4 - b) * stride_b

    def piece(owner, c):
        mat, off = CHUNKS[c]
        return outs[mat].at[pl.ds(pl.multiple_of(owner * ROWS + off, PIECE), PIECE)]

    n = len(CHUNKS)
    links = {"A+": at_a(a + 1), "A-": at_a(a + 3), "B+": at_b(b + 1), "B-": at_b(b + 3)}
    have = {}
    count = [0]

    def pass_on(da, db, c):
        here = piece(block_row(da, db), c)
        for link in follow_ups(da, db, c):
            ra, rb = seen_by_receiver(link, da, db)
            start(remote(here, here, send_sem.at[count[0]], recv_sem.at[(ra * 4 + rb) * n + c],
                         (links[link], x)))
            count[0] += 1
        mat = CHUNKS[c][0]
        got = have.setdefault((da, db, mat), [])
        got.append(c)
        if len(got) == ROWS // PIECE:
            owner = block_row(da, db)
            block = outs[mat].at[pl.ds(pl.multiple_of(owner * ROWS, ROWS), ROWS)]
            k = (da * 4 + db) * 2 + mat
            start(remote(block, block, die_send.at[k], die_recv.at[k], (partner, x)))

    def make_chunk(c):
        mat, off = CHUNKS[c]
        scale = inverse[mat]
        for i in range(0, PIECE, 16):
            rows = pl.ds(pl.multiple_of(row * ROWS + off + i, 16), 16)
            outs[mat][rows, :] = (latest[mat][off + i : off + i + 16, :] * scale).astype(
                jnp.bfloat16
            )

    norm_at = {8: 0, 16: 1, 24: 2, 32: 3}
    for i, (da, db, c) in enumerate(ORDER):
        if i in norm_at:
            s = norm_at[i]
            if s < 3:
                total = norm_wait(s, (x, y, z)[s])
            if s == 0:
                nslots[1, y] = total
                norm_stage(1, lambda d: (at_y(y + d), x), y)
            elif s == 1:
                nslots[2, z] = total
                norm_stage(2, lambda d: (at_z(z + d), x), z)
            elif s == 2:
                nslots[3, 0] = total
                start(remote(nslots.at[3, 0], nslots.at[3, 1], n_send.at[9], n_recv.at[9],
                             (partner, x)))
            else:
                remote(nslots.at[3, 1], nslots.at[3, 1], n_send.at[9], n_recv.at[9],
                       (partner, x)).wait_recv()
                norm_out[...] = (nslots[3, 0] + nslots[3, 1]).astype(jnp.bfloat16)
        if (da, db) == (0, 0):
            make_chunk(c)
        else:
            here = piece(block_row(da, db), c)
            remote(here, here, send_sem.at[0], recv_sem.at[(da * 4 + db) * n + c],
                   (partner, x)).wait_recv()
        pass_on(da, db, c)

    for pa in range(4):
        for pb in range(4):
            owner = partner + ((b + pa) % 4 - b) * stride_b + ((a + pb) % 4 - a) * stride_a
            for mat in range(2):
                block = outs[mat].at[pl.ds(pl.multiple_of(owner * ROWS, ROWS), ROWS)]
                k = (pa * 4 + pb) * 2 + mat
                remote(block, block, die_send.at[k], die_recv.at[k], (partner, x)).wait_recv()
    for copy in sent:
        copy.wait_send()


N_SENDS = sum(len(follow_ups(*item)) for item in ORDER)


def gather(*args):
    f32, bf16 = jnp.float32, jnp.bfloat16
    dma = pltpu.SemaphoreType.DMA
    anywhere = pl.BlockSpec(memory_space=pl.ANY)
    on_chip = pl.BlockSpec(memory_space=pltpu.VMEM)
    return pl.pallas_call(
        gather_kernel,
        name="gather_kernel",
        out_shape=[
            pltpu.VMEM((D_MODEL, WIDTH), bf16),
            pltpu.VMEM((D_MODEL, WIDTH), bf16),
            pltpu.VMEM((1, WIDTH), f32),
            pltpu.VMEM((1, WIDTH), f32),
            pltpu.VMEM((16, 128), bf16),
            pltpu.VMEM((ROWS, WIDTH), f32),
            pltpu.VMEM((ROWS, WIDTH), f32),
        ],
        in_specs=[anywhere] * 6 + [on_chip],
        out_specs=[on_chip] * 7,
        scratch_shapes=[
            pltpu.VMEM((2, ROWS, WIDTH), f32),
            pltpu.VMEM((2, ROWS, WIDTH), f32),
            pltpu.VMEM((2, 1, WIDTH), f32),
            pltpu.VMEM((2, 1, WIDTH), f32),
            pltpu.VMEM((2, 1, WIDTH), f32),
            pltpu.VMEM((2, 2, 4, 1, WIDTH), f32),
            pltpu.VMEM((4, 4, 16, 128), f32),
            dma((6,)),
            dma((N_SENDS,)),
            dma((16 * len(CHUNKS),)),
            dma((32,)),
            dma((32,)),
            dma((13,)),
            dma((13,)),
            dma((10,)),
            dma((10,)),
        ],
        compiler_params=pltpu.CompilerParams(
            collective_id=0, has_side_effects=True, vmem_limit_bytes=30 * 1024 * 1024
        ),
    )(*(pltpu.with_memory_space_constraint(v, pltpu.HBM) for v in args[:6]), *args[6:])


def write_kernel(*refs):
    k = len(refs) // 2
    srcs, dsts, sem = refs[:k], refs[k : 2 * k], refs[2 * k]
    copies, count = [], 0
    for src, dst in zip(srcs, dsts):
        pieces = 4 if src.shape[0] == D_MODEL else 1
        rows = src.shape[0] // pieces
        for p in range(pieces):
            at = pl.ds(p * rows, rows)
            copies.append(pltpu.make_async_copy(src.at[at], dst.at[at], sem.at[count]))
            count += 1
    for copy in copies:
        copy.start()
    for copy in copies:
        copy.wait()


def write(arrays):
    anywhere = pl.BlockSpec(memory_space=pl.ANY)
    return pl.pallas_call(
        write_kernel,
        name="write_kernel",
        out_shape=[jax.ShapeDtypeStruct(v.shape, v.dtype) for v in arrays],
        in_specs=[anywhere] * len(arrays),
        out_specs=[anywhere] * len(arrays),
        scratch_shapes=[pltpu.SemaphoreType.DMA((16,))],
        compiler_params=pltpu.CompilerParams(vmem_limit_bytes=1024 * 1024),
    )(*arrays)


def local(w_gate, first_gate, second_gate, w_up, first_up, second_up, norm_train, norm_step):
    device = lax.axis_index("rows") * 4 + lax.axis_index("cols")
    gain = jnp.tile(norm_train + norm_step, 128).reshape(16, 128)
    slot = lax.broadcasted_iota(jnp.int32, (16, 128), 0) * 8
    slot = slot + lax.broadcasted_iota(jnp.int32, (16, 128), 1) // 16
    placed = jnp.where(slot == device, gain, 0.0)
    held = gather(w_gate, first_gate, second_gate, w_up, first_up, second_up, placed)
    ready_g, ready_u, col_g, col_u, norm, latest_g, latest_u = write(held)
    return (
        ready_g,
        ready_u,
        col_g.reshape(WIDTH),
        col_u.reshape(WIDTH),
        norm.reshape(D_MODEL),
        latest_g,
        latest_u,
    )


def solution(mesh):
    split = P("rows", "cols")
    return jax.shard_map(
        local,
        mesh=mesh,
        in_specs=(split,) * 6 + (P(("rows", "cols")),) * 2,
        out_specs=(P(None, "cols"),) * 2 + (P("cols"),) * 2 + (P(),) + (split,) * 2,
        check_vma=False,
    )
```

```python
import heapq

import jax
import jax.numpy as jnp
from jax import lax
from jax.experimental import pallas as pl
from jax.experimental.pallas import tpu as pltpu
from jax.sharding import PartitionSpec as P

D_MODEL = 2048
WIDTH = 2048
ROWS = 64
SIDE = 4
MESH = pl.DeviceIdType.MESH

learn_rate = 0.01
decay_rate = 0.1
tiny_value = 1e-08

CHUNKS = ((0, 0, 32), (1, 0, 32), (0, 32, 32), (1, 32, 32))
N = len(CHUNKS)
RAW = (0,)
LOW = (0, 1)
HIGH = (2, 3)
RAW_ROWS = 8
LINKS = ("A+", "A-", "B+", "B-")
NEIGHBOURS = {"A+": (3, 0), "A-": (1, 0), "B+": (0, 3), "B-": (0, 1)}
FINE_TAIL = 14


def follow_ups(da, db, c):
    if (da, db) == (0, 0):
        return () if c in RAW else LINKS
    if db == 0:
        on = ("B+", "B-")
        if da == 3 and c in LOW:
            on = ("A+",) + on
        if da == 1 and c in HIGH:
            on = ("A-",) + on
        return on
    if db == 3 and c in LOW:
        return ("B+",)
    if db == 1 and c in HIGH:
        return ("B-",)
    return ()


def seen_by_receiver(link, da, db):
    step = -1 if link[1] == "+" else 1
    return ((da + step) % 4, db) if link[0] == "A" else (da, (db + step) % 4)


def arrival_order():
    delay = 1.4
    queues = {k: [] for k in LINKS}
    done = {k: 0.0 for k in queues}
    first = [(0, 0, c) for c in range(N) if c not in RAW]
    first += [NEIGHBOURS[k] + (c,) for c in RAW for k in LINKS]
    first += [(0, 0, c) for c in RAW]
    events = [(0.0, i, item) for i, item in enumerate(first)]
    order, now, serial = [], 0.0, len(first)
    while events or any(queues.values()):
        rate = {}
        for k in queues:
            if queues[k]:
                other = ("B" if k[0] == "A" else "A") + k[1]
                size = CHUNKS[queues[k][0][2]][2] / 32
                rate[k] = (0.5 if queues[other] else 1.0) / size
        steps = [(1 - done[k]) / rate[k] for k in rate]
        if events:
            steps.append(events[0][0] - now)
        dt = max(0.0, min(steps))
        now += dt
        for k in rate:
            done[k] += rate[k] * dt
            if done[k] >= 1 - 1e-9:
                da, db, c = queues[k].pop(0)
                done[k] = 0.0
                serial += 1
                heapq.heappush(events, (now + delay, serial, seen_by_receiver(k, da, db) + (c,)))
        while events and events[0][0] <= now + 1e-9:
            item = heapq.heappop(events)[2]
            order.append(item)
            for k in follow_ups(*item):
                queues[k].append(item)
    return order


def group_of(da, db, c):
    if (da, db) in NEIGHBOURS.values() and c in RAW:
        return ("raw", db == 0, c)
    if db == 0:
        return ("A", da % 2, c if da != 2 else c % 2)
    return ("B", da, db % 2, c if db != 2 else c % 2)


def die_copies(order):
    copies, waiting, seen = [], {}, {}
    last = {}
    for i, item in enumerate(order):
        last[item if item[:2] == (0, 0) else group_of(*item)] = i
    at = [(last[e if e[:2] == (0, 0) else group_of(*e)], e) for e in order]
    for i, (da, db, c) in sorted(at, key=lambda v: v[0]):
        mat, off, rows = CHUNKS[c]
        held = waiting.setdefault((da, db, mat), [])
        held.append((off, rows))
        seen[da, db, mat] = seen.get((da, db, mat), 0) + rows
        if i >= len(order) - FINE_TAIL:
            copies += [(i, da, db, mat, *piece) for piece in held]
            held.clear()
        elif seen[da, db, mat] == ROWS:
            copies.append((i, da, db, mat, 0, ROWS))
            held.clear()
    return copies


ORDER = arrival_order()
DIE = die_copies(ORDER)
SENT_ROWS = sum(len(follow_ups(*item)) * CHUNKS[item[2]][2] for item in ORDER)
RAW_TOTAL = sum(CHUNKS[c][2] for c in RAW)


GROUPS = {}
for _item in ORDER:
    if _item[:2] != (0, 0):
        GROUPS.setdefault(group_of(*_item), []).append(_item)
GROUP_NUMBER = {g: i for i, g in enumerate(GROUPS)}


def gather_kernel(
    w_g, f_g, s_g, w_u, f_u, s_u, n_t, n_s,
    out_g, out_u, col_g, col_u, norm_out, latest_g, latest_u,
    first, second, part, pair, inverse, slots, nslots, n_in, raw,
    load_sem, send_sem, recv_sem, raw_send, die_send, die_recv,
    sum_send, sum_recv, n_send, n_recv,
):
    row = lax.axis_index("rows")
    x = lax.axis_index("cols")
    core = row % 2
    y = (row // 2) % 4
    z = row // 8
    a = y * (1 - core) + z * core
    b = z * (1 - core) + y * core
    stride_a = 2 + 6 * core
    stride_b = 8 - 6 * core
    partner = row + 1 - 2 * core
    outs = (out_g, out_u)
    latest = (latest_g, latest_u)

    def at_a(pos):
        return row + ((pos % 4) - a) * stride_a

    def at_b(pos):
        return row + ((pos % 4) - b) * stride_b

    def at_y(pos):
        return row + ((pos % 4) - y) * 2

    def at_z(pos):
        return row + ((pos % 4) - z) * 8

    half = ROWS // 2

    def first_of(m):
        return first.at[pl.ds(m * ROWS, ROWS)]

    for m, (w, f, s) in enumerate(((w_g, f_g, s_g), (w_u, f_u, s_u))):
        for h in range(2):
            at = pl.ds(h * half, half)
            for src, dst in ((w, latest[m]), (f, first_of(m)), (s, second.at[m])):
                copy = pltpu.make_async_copy(
                    src.at[at], dst.at[at], load_sem.at[2 * m + h]
                )
                copy.start()
    for j, src in enumerate((n_t, n_s)):
        pltpu.make_async_copy(src, n_in.at[j], load_sem.at[4]).start()

    barrier = pltpu.get_barrier_semaphore()
    peers = [(partner, x)]
    for d in range(1, 4):
        peers += [(at_y(y + d), x), (at_z(z + d), x), (row, (x + d) % 4)]
    for peer in peers:
        pl.semaphore_signal(barrier, inc=1, device_id=peer, device_id_type=MESH)

    for m in range(2):
        acc = jnp.zeros((8, WIDTH), jnp.float32)
        for h in range(2):
            three = first.at[pl.ds(0, 3 * half)]
            pltpu.make_async_copy(three, three, load_sem.at[2 * m + h]).wait()

            def step(i, acc, m=m):
                at = pl.ds(pl.multiple_of(i * 8, 8), 8)
                w = latest[m][at, :]
                new = w - learn_rate * (
                    first_of(m)[at, :] / (jnp.sqrt(second[m, at, :]) + tiny_value) + decay_rate * w
                )
                latest[m][at, :] = new
                return acc + jnp.abs(new)

            acc = lax.fori_loop(h * half // 8, (h + 1) * half // 8, step, acc)
        part[m] = jnp.sum(acc, axis=0, keepdims=True)

    pl.semaphore_wait(barrier, len(peers))

    def remote(src, dst, send, recv, device):
        return pltpu.make_async_remote_copy(
            src_ref=src, dst_ref=dst, send_sem=send, recv_sem=recv,
            device_id=device, device_id_type=MESH,
        )

    def start(src, dst, send, recv, device):
        remote(src, dst, send, recv, device).start()

    def arrived(ref, recv):
        remote(ref, ref, send_sem, recv, (partner, x)).wait_recv()

    def left(ref, send):
        remote(ref, ref, send, die_recv, (partner, x)).wait_send()

    links = {
        "A+": (at_a(a + 1), x), "A-": (at_a(a + 3), x),
        "B+": (at_b(b + 1), x), "B-": (at_b(b + 3), x),
    }
    raw_pieces = [(c, p) for c in RAW for p in range(0, CHUNKS[c][2], RAW_ROWS)]

    raw_row = {c: sum(CHUNKS[e][2] for e in RAW[:j]) for j, c in enumerate(RAW)}

    def send_raw(number):
        for _ in range(number):
            if not raw_pieces:
                return
            c, p = raw_pieces.pop(0)
            mat, off, _ = CHUNKS[c]
            for i, k in enumerate(LINKS):
                start(latest[mat].at[pl.ds(off + p, RAW_ROWS)],
                      raw.at[i, pl.ds(raw_row[c] + p, RAW_ROWS)], raw_send,
                      recv_sem.at[GROUP_NUMBER[group_of(*NEIGHBOURS[k], c)]], links[k])

    start(part, pair, sum_send, sum_recv.at[0], (partner, x))
    send_raw(RAW_BEFORE[0])

    def norm_stage(i, device_of, me):
        mine = nslots.at[4 * i + me]
        for d in range(1, 4):
            start(mine, mine, n_send, n_recv.at[i], device_of(d))

    def norm_wait(i):
        arrived(nslots.at[pl.ds(0, 3)], n_recv.at[i])
        total = nslots[4 * i]
        for k in range(1, 4):
            total = total + nslots[4 * i + k]
        return total

    pltpu.make_async_copy(n_in, n_in, load_sem.at[4]).wait()
    gain = n_in[0] + n_in[1]
    gain = jnp.broadcast_to(jnp.concatenate([gain] * 8, axis=1), (16, 128))
    place = lax.broadcasted_iota(jnp.int32, (16, 128), 0) * 8
    place = place + lax.broadcasted_iota(jnp.int32, (16, 128), 1) // 16
    nslots[x] = jnp.where(place == row * 4 + x, gain, 0.0)

    arrived(pair, sum_recv.at[0])
    places = ((y, z), (z, y))
    movers = ((at_y, at_z), (at_z, at_y))
    for m in range(2):
        slots[4 * m + places[m][0]] = part[m] + pair[m]
    for stage in range(2):
        for d in range(1, 4):
            for m in range(2):
                me = places[m][stage]
                mine = slots.at[8 * stage + 4 * m + me]
                start(mine, mine, sum_send, sum_recv.at[1 + stage], (movers[m][stage](me + d), x))
        send_raw(RAW_BEFORE[1 + stage])
        arrived(slots.at[pl.ds(0, 6)], sum_recv.at[1 + stage])
        for m in range(2):
            total = slots[8 * stage + 4 * m]
            for k in range(1, 4):
                total = total + slots[8 * stage + 4 * m + k]
            if stage == 0:
                slots[8 + 4 * m + places[m][1]] = total
            else:
                column = total * (1.0 / D_MODEL)
                (col_g, col_u)[m][...] = column
                inverse[m] = 1.0 / column
    norm_stage(0, lambda d: (row, (x + d) % 4), x)

    def block_row(da, db):
        return row + ((a + da) % 4 - a) * stride_a + ((b + db) % 4 - b) * stride_b

    def rows_of(owner, mat, off, rows):
        return outs[mat].at[pl.ds(pl.multiple_of(owner * ROWS + off, 16), rows)]

    passed = [0]

    def pass_on(da, db, c):
        here = rows_of(block_row(da, db), *CHUNKS[c])
        for link in follow_ups(da, db, c):
            group = group_of(*seen_by_receiver(link, da, db), c)
            start(here, here, send_sem, recv_sem.at[GROUP_NUMBER[group]], links[link])

    def pass_over(i):
        while passed[0] < len(DIE) and DIE[passed[0]][0] == i:
            _, ea, eb, mat, off, rows = DIE[passed[0]]
            block = rows_of(block_row(ea, eb), mat, off, rows)
            start(block, block, die_send, die_recv, (partner, x))
            passed[0] += 1

    def scaled(value, mat):
        return (value * inverse[mat]).astype(jnp.bfloat16)

    def norm_step(s):
        if s == 3:
            arrived(nslots.at[13], n_recv.at[3])
            norm_out[...] = (nslots[12] + nslots[13]).astype(jnp.bfloat16)
            return
        total = norm_wait(s)
        if s == 0:
            nslots[4 + y] = total
            norm_stage(1, lambda d: (at_y(y + d), x), y)
        elif s == 1:
            nslots[8 + z] = total
            norm_stage(2, lambda d: (at_z(z + d), x), z)
        else:
            nslots[12] = total
            start(nslots.at[12], nslots.at[13], n_send, n_recv.at[3], (partner, x))

    waiting = {g: list(members) for g, members in GROUPS.items()}
    norm_at = [NORM_FIRST + NORM_EVERY * k for k in range(4)]
    for i, (da, db, c) in enumerate(ORDER):
        if i in norm_at:
            norm_step(norm_at.index(i))
        mat, off, rows = CHUNKS[c]
        if (da, db) == (0, 0):
            for p in range(0, rows, 16):
                at = pl.ds(pl.multiple_of(row * ROWS + off + p, 16), 16)
                outs[mat][at, :] = scaled(latest[mat][off + p : off + p + 16, :], mat)
            pass_on(da, db, c)
            pass_over(i)
            continue
        group = group_of(da, db, c)
        waiting[group].remove((da, db, c))
        if waiting[group]:
            continue
        total = sum(CHUNKS[e][2] for _, _, e in GROUPS[group])
        if group[0] == "raw":
            arrived(first.at[pl.ds(0, total)], recv_sem.at[GROUP_NUMBER[group]])
        else:
            arrived(outs[0].at[pl.ds(0, total)], recv_sem.at[GROUP_NUMBER[group]])
        for ea, eb, e in GROUPS[group]:
            mat, off, rows = CHUNKS[e]
            if group[0] == "raw":
                k = list(NEIGHBOURS.values()).index((ea, eb))
                for p in range(0, rows, 16):
                    at = pl.ds(pl.multiple_of(block_row(ea, eb) * ROWS + off + p, 16), 16)
                    outs[mat][at, :] = scaled(raw[k, raw_row[e] + p : raw_row[e] + p + 16, :], mat)
            pass_on(ea, eb, e)
        pass_over(i)

    arrived(outs[0], die_recv)
    left(outs[0], die_send)
    left(outs[0].at[pl.ds(0, SENT_ROWS)], send_sem)
    left(first.at[pl.ds(0, 4 * RAW_TOTAL)], raw_send)
    left(slots.at[pl.ds(0, 14)], sum_send)
    left(nslots.at[pl.ds(0, 10)], n_send)


NORM_FIRST, NORM_EVERY = 12, 10
RAW_BEFORE = (1, 2, 1)


def gather(*args):
    f32, bf16 = jnp.float32, jnp.bfloat16
    dma = pltpu.SemaphoreType.DMA
    anywhere = pl.BlockSpec(memory_space=pl.ANY)
    on_chip = pl.BlockSpec(memory_space=pltpu.VMEM)
    return pl.pallas_call(
        gather_kernel,
        name="gather_kernel",
        out_shape=[
            pltpu.VMEM((D_MODEL, WIDTH), bf16),
            pltpu.VMEM((D_MODEL, WIDTH), bf16),
            pltpu.VMEM((1, WIDTH), f32),
            pltpu.VMEM((1, WIDTH), f32),
            pltpu.VMEM((16, 128), bf16),
            pltpu.VMEM((ROWS, WIDTH), f32),
            pltpu.VMEM((ROWS, WIDTH), f32),
        ],
        in_specs=[anywhere] * 8,
        out_specs=[on_chip] * 7,
        scratch_shapes=[
            pltpu.VMEM((2 * ROWS, WIDTH), f32),
            pltpu.VMEM((2, ROWS, WIDTH), f32),
            pltpu.VMEM((2, 1, WIDTH), f32),
            pltpu.VMEM((2, 1, WIDTH), f32),
            pltpu.VMEM((2, 1, WIDTH), f32),
            pltpu.VMEM((16, 1, WIDTH), f32),
            pltpu.VMEM((16, 16, 128), f32),
            pltpu.VMEM((2, 1, 16), f32),
            pltpu.VMEM((4, RAW_TOTAL, WIDTH), f32),
            dma((5,)),
            dma,
            dma((len(GROUPS),)),
            dma,
            dma,
            dma,
            dma,
            dma((3,)),
            dma,
            dma((4,)),
        ],
        compiler_params=pltpu.CompilerParams(
            collective_id=0, has_side_effects=True, vmem_limit_bytes=30 * 1024 * 1024
        ),
    )(*(pltpu.with_memory_space_constraint(v, pltpu.HBM) for v in args))


def write_kernel(*refs):
    k = len(refs) // 2
    srcs, dsts, sem = refs[:k], refs[k : 2 * k], refs[2 * k]
    copies, count = [], 0
    for src, dst in zip(srcs, dsts):
        pieces = WRITE_PIECES if src.shape[0] == D_MODEL else 1
        rows = src.shape[0] // pieces
        for p in range(pieces):
            at = pl.ds(p * rows, rows)
            copies.append(pltpu.make_async_copy(src.at[at], dst.at[at], sem.at[count]))
            count += 1
    for copy in copies:
        copy.start()
    for copy in copies:
        copy.wait()


WRITE_PIECES = 4


def write(arrays):
    anywhere = pl.BlockSpec(memory_space=pl.ANY)
    return pl.pallas_call(
        write_kernel,
        name="write_kernel",
        out_shape=[jax.ShapeDtypeStruct(v.shape, v.dtype) for v in arrays],
        in_specs=[anywhere] * len(arrays),
        out_specs=[anywhere] * len(arrays),
        scratch_shapes=[pltpu.SemaphoreType.DMA((2 * WRITE_PIECES + 5,))],
        compiler_params=pltpu.CompilerParams(vmem_limit_bytes=1024 * 1024),
    )(*arrays)


def local(w_gate, first_gate, second_gate, w_up, first_up, second_up, norm_train, norm_step):
    norms = (norm_train.reshape(1, 16), norm_step.reshape(1, 16))
    held = gather(w_gate, first_gate, second_gate, w_up, first_up, second_up, *norms)
    ready_g, ready_u, col_g, col_u, norm, latest_g, latest_u = write(held)
    return (
        ready_g,
        ready_u,
        col_g.reshape(WIDTH),
        col_u.reshape(WIDTH),
        norm.reshape(D_MODEL),
        latest_g,
        latest_u,
    )


def solution(mesh):
    split = P("rows", "cols")
    return jax.shard_map(
        local,
        mesh=mesh,
        in_specs=(split,) * 6 + (P(("rows", "cols")),) * 2,
        out_specs=(P(None, "cols"),) * 2 + (P("cols"),) * 2 + (P(),) + (split,) * 2,
        check_vma=False,
    )
```

```python
import heapq

import jax
import jax.numpy as jnp
from jax import lax
from jax.experimental import pallas as pl
from jax.experimental.pallas import tpu as pltpu
from jax.sharding import PartitionSpec as P

D_MODEL = 2048
WIDTH = 2048
ROWS = 64
SIDE = 4
MESH = pl.DeviceIdType.MESH

learn_rate = 0.01
decay_rate = 0.1
tiny_value = 1e-08

CHUNKS = ((0, 0, 32), (1, 0, 32), (0, 32, 32), (1, 32, 32))
N = len(CHUNKS)
RAW = (0,)
LOW = (0, 1)
HIGH = (2, 3)
RAW_ROWS = 8
LINKS = ("A+", "A-", "B+", "B-")
NEIGHBOURS = {"A+": (3, 0), "A-": (1, 0), "B+": (0, 3), "B-": (0, 1)}
FINE_TAIL = 14


def follow_ups(da, db, c):
    if (da, db) == (0, 0):
        return () if c in RAW else LINKS
    if db == 0:
        on = ("B+", "B-")
        if da == 3 and c in LOW:
            on = ("A+",) + on
        if da == 1 and c in HIGH:
            on = ("A-",) + on
        return on
    if db == 3 and c in LOW:
        return ("B+",)
    if db == 1 and c in HIGH:
        return ("B-",)
    return ()


def seen_by_receiver(link, da, db):
    step = -1 if link[1] == "+" else 1
    return ((da + step) % 4, db) if link[0] == "A" else (da, (db + step) % 4)


def arrival_order():
    delay = 1.4
    queues = {k: [] for k in LINKS}
    done = {k: 0.0 for k in queues}
    first = [(0, 0, c) for c in range(N) if c not in RAW]
    first += [NEIGHBOURS[k] + (c,) for c in RAW for k in LINKS]
    first += [(0, 0, c) for c in RAW]
    events = [(0.0, i, item) for i, item in enumerate(first)]
    order, now, serial = [], 0.0, len(first)
    while events or any(queues.values()):
        rate = {}
        for k in queues:
            if queues[k]:
                other = ("B" if k[0] == "A" else "A") + k[1]
                size = CHUNKS[queues[k][0][2]][2] / 32
                rate[k] = (0.5 if queues[other] else 1.0) / size
        steps = [(1 - done[k]) / rate[k] for k in rate]
        if events:
            steps.append(events[0][0] - now)
        dt = max(0.0, min(steps))
        now += dt
        for k in rate:
            done[k] += rate[k] * dt
            if done[k] >= 1 - 1e-9:
                da, db, c = queues[k].pop(0)
                done[k] = 0.0
                serial += 1
                heapq.heappush(events, (now + delay, serial, seen_by_receiver(k, da, db) + (c,)))
        while events and events[0][0] <= now + 1e-9:
            item = heapq.heappop(events)[2]
            order.append(item)
            for k in follow_ups(*item):
                queues[k].append(item)
    return order


def group_of(da, db, c):
    if (da, db) in NEIGHBOURS.values() and c in RAW:
        return ("raw", db == 0, c)
    if db == 0:
        return ("A", da % 2, c if da != 2 else c % 2)
    return ("B", da, db % 2, c if db != 2 else c % 2)


def die_copies(order):
    copies, waiting, seen = [], {}, {}
    last = {}
    for i, item in enumerate(order):
        last[item if item[:2] == (0, 0) else group_of(*item)] = i
    at = [(last[e if e[:2] == (0, 0) else group_of(*e)], e) for e in order]
    for i, (da, db, c) in sorted(at, key=lambda v: v[0]):
        mat, off, rows = CHUNKS[c]
        held = waiting.setdefault((da, db, mat), [])
        held.append((off, rows))
        seen[da, db, mat] = seen.get((da, db, mat), 0) + rows
        if i >= len(order) - FINE_TAIL:
            copies += [(i, da, db, mat, *piece) for piece in held]
            held.clear()
        elif seen[da, db, mat] == ROWS:
            copies.append((i, da, db, mat, 0, ROWS))
            held.clear()
    return copies


ORDER = arrival_order()
DIE = die_copies(ORDER)
SENT_ROWS = sum(len(follow_ups(*item)) * CHUNKS[item[2]][2] for item in ORDER)
RAW_TOTAL = sum(CHUNKS[c][2] for c in RAW)


GROUPS = {}
for _item in ORDER:
    if _item[:2] != (0, 0):
        GROUPS.setdefault(group_of(*_item), []).append(_item)
GROUP_NUMBER = {g: i for i, g in enumerate(GROUPS)}


def gather_kernel(
    w_g, f_g, s_g, w_u, f_u, s_u, n_t, n_s,
    out_g, out_u, col_g, col_u, norm_out, latest_g, latest_u,
    first, second, inverse, slots, nslots, n_in, raw,
    load_sem, send_sem, recv_sem, raw_send, die_send, die_recv,
    sum_send, sum_recv, n_send, n_recv,
):
    row = lax.axis_index("rows")
    x = lax.axis_index("cols")
    core = row % 2
    y = (row // 2) % 4
    z = row // 8
    a = y * (1 - core) + z * core
    b = z * (1 - core) + y * core
    stride_a = 2 + 6 * core
    stride_b = 8 - 6 * core
    partner = row + 1 - 2 * core
    outs = (out_g, out_u)
    latest = (latest_g, latest_u)

    def at_a(pos):
        return row + ((pos % 4) - a) * stride_a

    def at_b(pos):
        return row + ((pos % 4) - b) * stride_b

    def at_y(pos):
        return row + ((pos % 4) - y) * 2

    def at_z(pos):
        return row + ((pos % 4) - z) * 8

    places = ((y, z), (z, y))
    movers = ((at_y, at_z), (at_z, at_y))

    half = ROWS // 2

    def first_of(m):
        return first.at[pl.ds(m * ROWS, ROWS)]

    for m, (w, f, s) in enumerate(((w_g, f_g, s_g), (w_u, f_u, s_u))):
        for h in range(2):
            at = pl.ds(h * half, half)
            for src, dst in ((w, latest[m]), (f, first_of(m)), (s, second.at[m])):
                copy = pltpu.make_async_copy(
                    src.at[at], dst.at[at], load_sem.at[2 * m + h]
                )
                copy.start()
    for j, src in enumerate((n_t, n_s)):
        pltpu.make_async_copy(src, n_in.at[j], load_sem.at[4]).start()

    barrier = pltpu.get_barrier_semaphore()
    peers = [(partner, x)]
    for d in range(1, 4):
        peers += [(at_y(y + d), x), (at_z(z + d), x), (row, (x + d) % 4)]
        peers += [(at_y(y + d) + partner - row, x), (at_z(z + d) + partner - row, x)]
    for peer in peers:
        pl.semaphore_signal(barrier, inc=1, device_id=peer, device_id_type=MESH)

    for m in range(2):
        acc = jnp.zeros((8, WIDTH), jnp.float32)
        for h in range(2):
            three = first.at[pl.ds(0, 3 * half)]
            pltpu.make_async_copy(three, three, load_sem.at[2 * m + h]).wait()

            def step(i, acc, m=m):
                at = pl.ds(pl.multiple_of(i * 8, 8), 8)
                w = latest[m][at, :]
                new = w - learn_rate * (
                    first_of(m)[at, :] / (jnp.sqrt(second[m, at, :]) + tiny_value) + decay_rate * w
                )
                latest[m][at, :] = new
                return acc + jnp.abs(new)

            acc = lax.fori_loop(h * half // 8, (h + 1) * half // 8, step, acc, unroll=True)
        slots[8 * m + 2 * places[m][0] + core] = jnp.sum(acc, axis=0, keepdims=True)

    pl.semaphore_wait(barrier, len(peers))

    def remote(src, dst, send, recv, device):
        return pltpu.make_async_remote_copy(
            src_ref=src, dst_ref=dst, send_sem=send, recv_sem=recv,
            device_id=device, device_id_type=MESH,
        )

    def start(src, dst, send, recv, device):
        remote(src, dst, send, recv, device).start()

    def arrived(ref, recv):
        remote(ref, ref, send_sem, recv, (partner, x)).wait_recv()

    def left(ref, send):
        remote(ref, ref, send, die_recv, (partner, x)).wait_send()

    links = {
        "A+": (at_a(a + 1), x), "A-": (at_a(a + 3), x),
        "B+": (at_b(b + 1), x), "B-": (at_b(b + 3), x),
    }
    raw_pieces = [(c, p) for c in RAW for p in range(0, CHUNKS[c][2], RAW_ROWS)]

    raw_row = {c: sum(CHUNKS[e][2] for e in RAW[:j]) for j, c in enumerate(RAW)}

    def send_raw(number):
        for _ in range(number):
            if not raw_pieces:
                return
            c, p = raw_pieces.pop(0)
            mat, off, _ = CHUNKS[c]
            for i, k in enumerate(LINKS):
                start(latest[mat].at[pl.ds(off + p, RAW_ROWS)],
                      raw.at[i, pl.ds(raw_row[c] + p, RAW_ROWS)], raw_send,
                      recv_sem.at[GROUP_NUMBER[group_of(*NEIGHBOURS[k], c)]], links[k])

    for d in (2, 1, 3, 0):
        for m in range(2):
            mine = slots.at[8 * m + 2 * places[m][0] + core]
            there = movers[m][0](places[m][0] + d)
            start(mine, mine, sum_send, sum_recv.at[0], (there + partner - row, x))
            if d:
                start(mine, mine, sum_send, sum_recv.at[0], (there, x))
    send_raw(RAW_BEFORE[0])

    def norm_stage(i, device_of, me):
        mine = nslots.at[4 * i + me]
        for d in range(1, 4):
            start(mine, mine, n_send, n_recv.at[i], device_of(d))

    def norm_wait(i):
        arrived(nslots.at[pl.ds(0, 3)], n_recv.at[i])
        total = nslots[4 * i]
        for k in range(1, 4):
            total = total + nslots[4 * i + k]
        return total

    pltpu.make_async_copy(n_in, n_in, load_sem.at[4]).wait()
    gain = n_in[0] + n_in[1]
    gain = jnp.broadcast_to(jnp.concatenate([gain] * 8, axis=1), (16, 128))
    place = lax.broadcasted_iota(jnp.int32, (16, 128), 0) * 8
    place = place + lax.broadcasted_iota(jnp.int32, (16, 128), 1) // 16
    nslots[x] = jnp.where(place == row * 4 + x, gain, 0.0)

    for stage, count in enumerate((8, 4)):
        if stage == 1:
            for d in (2, 1, 3):
                for m in range(2):
                    mine = slots.at[16 + 4 * m + places[m][1]]
                    start(mine, mine, sum_send, sum_recv.at[1],
                          (movers[m][1](places[m][1] + d), x))
            send_raw(RAW_BEFORE[1])
        arrived(slots.at[pl.ds(0, (14, 6)[stage])], sum_recv.at[stage])
        for m in range(2):
            terms = [slots[16 * stage + count * m + k] for k in range(count)]
            while len(terms) > 1:
                terms = [p + q for p, q in zip(terms[::2], terms[1::2])]
            if stage == 0:
                slots[16 + 4 * m + places[m][1]] = terms[0]
            else:
                column = terms[0] * (1.0 / D_MODEL)
                (col_g, col_u)[m][...] = column
                inverse[m] = 1.0 / column
    norm_stage(0, lambda d: (row, (x + d) % 4), x)

    def block_row(da, db):
        return row + ((a + da) % 4 - a) * stride_a + ((b + db) % 4 - b) * stride_b

    def rows_of(owner, mat, off, rows):
        return outs[mat].at[pl.ds(pl.multiple_of(owner * ROWS + off, 16), rows)]

    passed = [0]

    def pass_on(da, db, c):
        here = rows_of(block_row(da, db), *CHUNKS[c])
        for link in follow_ups(da, db, c):
            group = group_of(*seen_by_receiver(link, da, db), c)
            start(here, here, send_sem, recv_sem.at[GROUP_NUMBER[group]], links[link])

    def pass_over(i):
        while passed[0] < len(DIE) and DIE[passed[0]][0] == i:
            _, ea, eb, mat, off, rows = DIE[passed[0]]
            block = rows_of(block_row(ea, eb), mat, off, rows)
            start(block, block, die_send, die_recv, (partner, x))
            passed[0] += 1

    def scaled(value, mat):
        return (value * inverse[mat]).astype(jnp.bfloat16)

    def norm_step(s):
        if s == 3:
            arrived(nslots.at[13], n_recv.at[3])
            norm_out[...] = (nslots[12] + nslots[13]).astype(jnp.bfloat16)
            return
        total = norm_wait(s)
        if s == 0:
            nslots[4 + y] = total
            norm_stage(1, lambda d: (at_y(y + d), x), y)
        elif s == 1:
            nslots[8 + z] = total
            norm_stage(2, lambda d: (at_z(z + d), x), z)
        else:
            nslots[12] = total
            start(nslots.at[12], nslots.at[13], n_send, n_recv.at[3], (partner, x))

    waiting = {g: list(members) for g, members in GROUPS.items()}
    norm_at = [NORM_FIRST + NORM_EVERY * k for k in range(4)]
    for i, (da, db, c) in enumerate(ORDER):
        if i in norm_at:
            norm_step(norm_at.index(i))
        mat, off, rows = CHUNKS[c]
        if (da, db) == (0, 0):
            for p in range(0, rows, 16):
                at = pl.ds(pl.multiple_of(row * ROWS + off + p, 16), 16)
                outs[mat][at, :] = scaled(latest[mat][off + p : off + p + 16, :], mat)
            pass_on(da, db, c)
            pass_over(i)
            continue
        group = group_of(da, db, c)
        waiting[group].remove((da, db, c))
        if waiting[group]:
            continue
        total = sum(CHUNKS[e][2] for _, _, e in GROUPS[group])
        if group[0] == "raw":
            arrived(first.at[pl.ds(0, total)], recv_sem.at[GROUP_NUMBER[group]])
        else:
            arrived(outs[0].at[pl.ds(0, total)], recv_sem.at[GROUP_NUMBER[group]])
        for ea, eb, e in GROUPS[group]:
            mat, off, rows = CHUNKS[e]
            if group[0] == "raw":
                k = list(NEIGHBOURS.values()).index((ea, eb))
                for p in range(0, rows, 16):
                    at = pl.ds(pl.multiple_of(block_row(ea, eb) * ROWS + off + p, 16), 16)
                    outs[mat][at, :] = scaled(raw[k, raw_row[e] + p : raw_row[e] + p + 16, :], mat)
            pass_on(ea, eb, e)
        pass_over(i)

    arrived(outs[0], die_recv)
    left(outs[0], die_send)
    left(outs[0].at[pl.ds(0, SENT_ROWS)], send_sem)
    left(raw, raw_send)
    left(slots.at[pl.ds(0, 20)], sum_send)
    left(nslots.at[pl.ds(0, 10)], n_send)


NORM_FIRST, NORM_EVERY = 12, 10
RAW_BEFORE = (2, 2)


def gather(*args):
    f32, bf16 = jnp.float32, jnp.bfloat16
    dma = pltpu.SemaphoreType.DMA
    anywhere = pl.BlockSpec(memory_space=pl.ANY)
    on_chip = pl.BlockSpec(memory_space=pltpu.VMEM)
    return pl.pallas_call(
        gather_kernel,
        name="gather_kernel",
        out_shape=[
            pltpu.VMEM((D_MODEL, WIDTH), bf16),
            pltpu.VMEM((D_MODEL, WIDTH), bf16),
            pltpu.VMEM((1, WIDTH), f32),
            pltpu.VMEM((1, WIDTH), f32),
            pltpu.VMEM((16, 128), bf16),
            pltpu.VMEM((ROWS, WIDTH), f32),
            pltpu.VMEM((ROWS, WIDTH), f32),
        ],
        in_specs=[anywhere] * 8,
        out_specs=[on_chip] * 7,
        scratch_shapes=[
            pltpu.VMEM((2 * ROWS, WIDTH), f32),
            pltpu.VMEM((2, ROWS, WIDTH), f32),
            pltpu.VMEM((2, 1, WIDTH), f32),
            pltpu.VMEM((24, 1, WIDTH), f32),
            pltpu.VMEM((16, 16, 128), f32),
            pltpu.VMEM((2, 1, 16), f32),
            pltpu.VMEM((4, RAW_TOTAL, WIDTH), f32),
            dma((5,)),
            dma,
            dma((len(GROUPS),)),
            dma,
            dma,
            dma,
            dma,
            dma((2,)),
            dma,
            dma((4,)),
        ],
        compiler_params=pltpu.CompilerParams(
            collective_id=0, has_side_effects=True, vmem_limit_bytes=30 * 1024 * 1024
        ),
    )(*(pltpu.with_memory_space_constraint(v, pltpu.HBM) for v in args))


def write_kernel(*refs):
    k = len(refs) // 2
    srcs, dsts, sem = refs[:k], refs[k : 2 * k], refs[2 * k]
    copies, count = [], 0
    for src, dst in zip(srcs, dsts):
        pieces = WRITE_PIECES if src.shape[0] == D_MODEL else 1
        rows = src.shape[0] // pieces
        for p in range(pieces):
            at = pl.ds(p * rows, rows)
            copies.append(pltpu.make_async_copy(src.at[at], dst.at[at], sem.at[count]))
            count += 1
    for copy in copies:
        copy.start()
    for copy in copies:
        copy.wait()


WRITE_PIECES = 4


def write(arrays):
    anywhere = pl.BlockSpec(memory_space=pl.ANY)
    return pl.pallas_call(
        write_kernel,
        name="write_kernel",
        out_shape=[jax.ShapeDtypeStruct(v.shape, v.dtype) for v in arrays],
        in_specs=[anywhere] * len(arrays),
        out_specs=[anywhere] * len(arrays),
        scratch_shapes=[pltpu.SemaphoreType.DMA((2 * WRITE_PIECES + 5,))],
        compiler_params=pltpu.CompilerParams(vmem_limit_bytes=1024 * 1024),
    )(*arrays)


def local(w_gate, first_gate, second_gate, w_up, first_up, second_up, norm_train, norm_step):
    norms = (norm_train.reshape(1, 16), norm_step.reshape(1, 16))
    held = gather(w_gate, first_gate, second_gate, w_up, first_up, second_up, *norms)
    ready_g, ready_u, col_g, col_u, norm, latest_g, latest_u = write(held)
    return (
        ready_g,
        ready_u,
        col_g.reshape(WIDTH),
        col_u.reshape(WIDTH),
        norm.reshape(D_MODEL),
        latest_g,
        latest_u,
    )


def solution(mesh):
    split = P("rows", "cols")
    return jax.shard_map(
        local,
        mesh=mesh,
        in_specs=(split,) * 6 + (P(("rows", "cols")),) * 2,
        out_specs=(P(None, "cols"),) * 2 + (P("cols"),) * 2 + (P(),) + (split,) * 2,
        check_vma=False,
    )
```

```python
import heapq

import jax
import jax.numpy as jnp
from jax import lax
from jax.experimental import pallas as pl
from jax.experimental.pallas import tpu as pltpu
from jax.sharding import PartitionSpec as P

D_MODEL = 2048
WIDTH = 2048
ROWS = 64
SIDE = 4
MESH = pl.DeviceIdType.MESH

learn_rate = 0.01
decay_rate = 0.1
tiny_value = 1e-08

CHUNKS = ((0, 0, 32), (1, 0, 16), (1, 16, 16), (0, 32, 32), (1, 32, 16), (1, 48, 16))
N = len(CHUNKS)
LOW = (0, 1, 2)
HIGH = (3, 4, 5)
FAR = (0, 1, 2, 0, 1, 2)
RAW_ROWS = 8
LINKS = ("A+", "A-", "B+", "B-")
NEIGHBOURS = {"A+": (3, 0), "A-": (1, 0), "B+": (0, 3), "B-": (0, 1)}
RAW = {0: LINKS, 1: ("A+", "A-")}
FINE_TAIL = 14


def follow_ups(da, db, c):
    if (da, db) == (0, 0):
        return tuple(k for k in LINKS if k not in RAW.get(c, ()))
    if db == 0:
        on = ("B+", "B-")
        if da == 3 and c in LOW:
            on = ("A+",) + on
        if da == 1 and c in HIGH:
            on = ("A-",) + on
        return on
    if db == 3 and c in LOW:
        return ("B+",)
    if db == 1 and c in HIGH:
        return ("B-",)
    return ()


def seen_by_receiver(link, da, db):
    step = -1 if link[1] == "+" else 1
    return ((da + step) % 4, db) if link[0] == "A" else (da, (db + step) % 4)


def arrival_order():
    delay = 1.4
    queues = {k: [] for k in LINKS}
    done = {k: 0.0 for k in queues}
    first = sorted([(0, 0, c) for c in range(N)], key=lambda v: len(RAW.get(v[2], ())) == 4)
    spot = len(first) - sum(len(k) == 4 for k in RAW.values())
    first[spot:spot] = [NEIGHBOURS[k] + (c,) for c in RAW for k in RAW[c]]
    events = [(0.0, i, item) for i, item in enumerate(first)]
    order, now, serial = [], 0.0, len(first)
    while events or any(queues.values()):
        rate = {}
        for k in queues:
            if queues[k]:
                other = ("B" if k[0] == "A" else "A") + k[1]
                size = CHUNKS[queues[k][0][2]][2] / 32
                rate[k] = (0.5 if queues[other] else 1.0) / size
        steps = [(1 - done[k]) / rate[k] for k in rate]
        if events:
            steps.append(events[0][0] - now)
        dt = max(0.0, min(steps))
        now += dt
        for k in rate:
            done[k] += rate[k] * dt
            if done[k] >= 1 - 1e-9:
                da, db, c = queues[k].pop(0)
                done[k] = 0.0
                serial += 1
                heapq.heappush(events, (now + delay, serial, seen_by_receiver(k, da, db) + (c,)))
        while events and events[0][0] <= now + 1e-9:
            item = heapq.heappop(events)[2]
            order.append(item)
            for k in follow_ups(*item):
                queues[k].append(item)
    return order


def group_of(da, db, c):
    if (da, db) in [NEIGHBOURS[k] for k in RAW.get(c, ())]:
        return ("raw", db == 0, c)
    if db == 0:
        return ("A", da % 2, c if da != 2 else FAR[c])
    return ("B", da, db % 2, c if db != 2 else FAR[c])


def die_copies(order):
    copies, waiting, seen = [], {}, {}
    last = {}
    for i, item in enumerate(order):
        last[item if item[:2] == (0, 0) else group_of(*item)] = i
    at = [(last[e if e[:2] == (0, 0) else group_of(*e)], e) for e in order]
    for i, (da, db, c) in sorted(at, key=lambda v: v[0]):
        mat, off, rows = CHUNKS[c]
        held = waiting.setdefault((da, db, mat), [])
        held.append((off, rows))
        seen[da, db, mat] = seen.get((da, db, mat), 0) + rows
        if i >= len(order) - FINE_TAIL:
            copies += [(i, da, db, mat, *piece) for piece in held]
            held.clear()
        elif seen[da, db, mat] == ROWS:
            copies.append((i, da, db, mat, 0, ROWS))
            held.clear()
    return copies


ORDER = arrival_order()
DIE = die_copies(ORDER)
SENT_ROWS = sum(len(follow_ups(*item)) * CHUNKS[item[2]][2] for item in ORDER)
RAW_TOTAL = sum(CHUNKS[c][2] * len(RAW[c]) for c in RAW)


GROUPS = {}
for _item in ORDER:
    if _item[:2] != (0, 0):
        GROUPS.setdefault(group_of(*_item), []).append(_item)
GROUP_NUMBER = {g: i for i, g in enumerate(GROUPS)}


def gather_kernel(
    w_g, f_g, s_g, w_u, f_u, s_u, n_t, n_s,
    out_g, out_u, col_g, col_u, norm_out, latest_g, latest_u,
    first, second, inverse, slots, nslots, n_in, raw,
    load_sem, send_sem, recv_sem, raw_send, die_send, die_recv,
    sum_send, sum_recv, n_send, n_recv,
):
    row = lax.axis_index("rows")
    x = lax.axis_index("cols")
    core = row % 2
    y = (row // 2) % 4
    z = row // 8
    a = y * (1 - core) + z * core
    b = z * (1 - core) + y * core
    stride_a = 2 + 6 * core
    stride_b = 8 - 6 * core
    partner = row + 1 - 2 * core
    outs = (out_g, out_u)
    latest = (latest_g, latest_u)

    def at_a(pos):
        return row + ((pos % 4) - a) * stride_a

    def at_b(pos):
        return row + ((pos % 4) - b) * stride_b

    def at_y(pos):
        return row + ((pos % 4) - y) * 2

    def at_z(pos):
        return row + ((pos % 4) - z) * 8

    places = ((y, z), (z, y))
    movers = ((at_y, at_z), (at_z, at_y))

    half = ROWS // 2

    def first_of(m):
        return first.at[pl.ds(m * ROWS, ROWS)]

    for m, (w, f, s) in enumerate(((w_g, f_g, s_g), (w_u, f_u, s_u))):
        for h in range(2):
            at = pl.ds(h * half, half)
            for src, dst in ((w, latest[m]), (f, first_of(m)), (s, second.at[m])):
                copy = pltpu.make_async_copy(
                    src.at[at], dst.at[at], load_sem.at[2 * m + h]
                )
                copy.start()
    for j, src in enumerate((n_t, n_s)):
        pltpu.make_async_copy(src, n_in.at[j], load_sem.at[4]).start()

    barrier = pltpu.get_barrier_semaphore()
    peers = [(partner, x)]
    for d in range(1, 4):
        peers += [(at_y(y + d), x), (at_z(z + d), x), (row, (x + d) % 4)]
        peers += [(at_y(y + d) + partner - row, x), (at_z(z + d) + partner - row, x)]
    for peer in peers:
        pl.semaphore_signal(barrier, inc=1, device_id=peer, device_id_type=MESH)

    for m in range(2):
        acc = jnp.zeros((8, WIDTH), jnp.float32)
        for h in range(2):
            three = first.at[pl.ds(0, 3 * half)]
            pltpu.make_async_copy(three, three, load_sem.at[2 * m + h]).wait()

            def step(i, acc, m=m):
                at = pl.ds(pl.multiple_of(i * 8, 8), 8)
                w = latest[m][at, :]
                new = w - learn_rate * (
                    first_of(m)[at, :] / (jnp.sqrt(second[m, at, :]) + tiny_value) + decay_rate * w
                )
                latest[m][at, :] = new
                return acc + jnp.abs(new)

            acc = lax.fori_loop(h * half // 8, (h + 1) * half // 8, step, acc, unroll=True)
        slots[8 * m + 2 * places[m][0] + core] = jnp.sum(acc, axis=0, keepdims=True)

    pl.semaphore_wait(barrier, len(peers))

    def remote(src, dst, send, recv, device):
        return pltpu.make_async_remote_copy(
            src_ref=src, dst_ref=dst, send_sem=send, recv_sem=recv,
            device_id=device, device_id_type=MESH,
        )

    def start(src, dst, send, recv, device):
        remote(src, dst, send, recv, device).start()

    def arrived(ref, recv):
        remote(ref, ref, send_sem, recv, (partner, x)).wait_recv()

    def left(ref, send):
        remote(ref, ref, send, die_recv, (partner, x)).wait_send()

    links = {
        "A+": (at_a(a + 1), x), "A-": (at_a(a + 3), x),
        "B+": (at_b(b + 1), x), "B-": (at_b(b + 3), x),
    }
    raw_pieces = [(c, p) for c in RAW for p in range(0, CHUNKS[c][2], RAW_ROWS)]

    raw_row, rows_so_far = {}, 0
    for c in RAW:
        for k in RAW[c]:
            raw_row[NEIGHBOURS[k] + (c,)] = rows_so_far
            rows_so_far += CHUNKS[c][2]

    def send_raw(number):
        for _ in range(number):
            if not raw_pieces:
                return
            c, p = raw_pieces.pop(0)
            mat, off, _ = CHUNKS[c]
            for k in RAW[c]:
                start(latest[mat].at[pl.ds(off + p, RAW_ROWS)],
                      raw.at[pl.ds(raw_row[NEIGHBOURS[k] + (c,)] + p, RAW_ROWS)], raw_send,
                      recv_sem.at[GROUP_NUMBER[group_of(*NEIGHBOURS[k], c)]], links[k])

    for d in (2, 1, 3, 0):
        for m in range(2):
            mine = slots.at[8 * m + 2 * places[m][0] + core]
            there = movers[m][0](places[m][0] + d)
            start(mine, mine, sum_send, sum_recv.at[0], (there + partner - row, x))
            if d:
                start(mine, mine, sum_send, sum_recv.at[0], (there, x))
    send_raw(RAW_BEFORE[0])

    def norm_stage(i, device_of, me):
        mine = nslots.at[4 * i + me]
        for d in range(1, 4):
            start(mine, mine, n_send, n_recv.at[i], device_of(d))

    def norm_wait(i):
        arrived(nslots.at[pl.ds(0, 3)], n_recv.at[i])
        total = nslots[4 * i]
        for k in range(1, 4):
            total = total + nslots[4 * i + k]
        return total

    pltpu.make_async_copy(n_in, n_in, load_sem.at[4]).wait()
    gain = n_in[0] + n_in[1]
    gain = jnp.broadcast_to(jnp.concatenate([gain] * 8, axis=1), (16, 128))
    place = lax.broadcasted_iota(jnp.int32, (16, 128), 0) * 8
    place = place + lax.broadcasted_iota(jnp.int32, (16, 128), 1) // 16
    nslots[x] = jnp.where(place == row * 4 + x, gain, 0.0)

    for stage, count in enumerate((8, 4)):
        if stage == 1:
            for d in (2, 1, 3):
                for m in range(2):
                    mine = slots.at[16 + 4 * m + places[m][1]]
                    start(mine, mine, sum_send, sum_recv.at[1],
                          (movers[m][1](places[m][1] + d), x))
            send_raw(RAW_BEFORE[1])
        arrived(slots.at[pl.ds(0, (14, 6)[stage])], sum_recv.at[stage])
        for m in range(2):
            terms = [slots[16 * stage + count * m + k] for k in range(count)]
            while len(terms) > 1:
                terms = [p + q for p, q in zip(terms[::2], terms[1::2])]
            if stage == 0:
                slots[16 + 4 * m + places[m][1]] = terms[0]
            else:
                column = terms[0] * (1.0 / D_MODEL)
                (col_g, col_u)[m][...] = column
                inverse[m] = 1.0 / column
    norm_stage(0, lambda d: (row, (x + d) % 4), x)

    def block_row(da, db):
        return row + ((a + da) % 4 - a) * stride_a + ((b + db) % 4 - b) * stride_b

    def rows_of(owner, mat, off, rows):
        return outs[mat].at[pl.ds(pl.multiple_of(owner * ROWS + off, 16), rows)]

    passed = [0]

    def pass_on(da, db, c):
        here = rows_of(block_row(da, db), *CHUNKS[c])
        for link in follow_ups(da, db, c):
            group = group_of(*seen_by_receiver(link, da, db), c)
            start(here, here, send_sem, recv_sem.at[GROUP_NUMBER[group]], links[link])

    def pass_over(i):
        while passed[0] < len(DIE) and DIE[passed[0]][0] == i:
            _, ea, eb, mat, off, rows = DIE[passed[0]]
            block = rows_of(block_row(ea, eb), mat, off, rows)
            start(block, block, die_send, die_recv, (partner, x))
            passed[0] += 1

    def scaled(value, mat):
        return (value * inverse[mat]).astype(jnp.bfloat16)

    def norm_step(s):
        if s == 3:
            arrived(nslots.at[13], n_recv.at[3])
            norm_out[...] = (nslots[12] + nslots[13]).astype(jnp.bfloat16)
            return
        total = norm_wait(s)
        if s == 0:
            nslots[4 + y] = total
            norm_stage(1, lambda d: (at_y(y + d), x), y)
        elif s == 1:
            nslots[8 + z] = total
            norm_stage(2, lambda d: (at_z(z + d), x), z)
        else:
            nslots[12] = total
            start(nslots.at[12], nslots.at[13], n_send, n_recv.at[3], (partner, x))

    waiting = {g: list(members) for g, members in GROUPS.items()}
    norm_at = [NORM_FIRST + NORM_EVERY * k for k in range(4)]
    for i, (da, db, c) in enumerate(ORDER):
        if i in norm_at:
            norm_step(norm_at.index(i))
        mat, off, rows = CHUNKS[c]
        if (da, db) == (0, 0):
            for p in range(0, rows, 16):
                at = pl.ds(pl.multiple_of(row * ROWS + off + p, 16), 16)
                outs[mat][at, :] = scaled(latest[mat][off + p : off + p + 16, :], mat)
            pass_on(da, db, c)
            pass_over(i)
            continue
        group = group_of(da, db, c)
        waiting[group].remove((da, db, c))
        if waiting[group]:
            continue
        total = sum(CHUNKS[e][2] for _, _, e in GROUPS[group])
        if group[0] == "raw":
            arrived(first.at[pl.ds(0, total)], recv_sem.at[GROUP_NUMBER[group]])
        else:
            arrived(outs[0].at[pl.ds(0, total)], recv_sem.at[GROUP_NUMBER[group]])
        for ea, eb, e in GROUPS[group]:
            mat, off, rows = CHUNKS[e]
            if group[0] == "raw":
                for p in range(0, rows, 16):
                    at = pl.ds(pl.multiple_of(block_row(ea, eb) * ROWS + off + p, 16), 16)
                    r = raw_row[ea, eb, e] + p
                    outs[mat][at, :] = scaled(raw[r : r + 16, :], mat)
            pass_on(ea, eb, e)
        pass_over(i)

    arrived(outs[0], die_recv)
    left(outs[0], die_send)
    left(outs[0].at[pl.ds(0, SENT_ROWS)], send_sem)
    left(raw, raw_send)
    left(slots.at[pl.ds(0, 20)], sum_send)
    left(nslots.at[pl.ds(0, 10)], n_send)


NORM_FIRST, NORM_EVERY = 12, 10
RAW_BEFORE = (3, 3)


def gather(*args):
    f32, bf16 = jnp.float32, jnp.bfloat16
    dma = pltpu.SemaphoreType.DMA
    anywhere = pl.BlockSpec(memory_space=pl.ANY)
    on_chip = pl.BlockSpec(memory_space=pltpu.VMEM)
    return pl.pallas_call(
        gather_kernel,
        name="gather_kernel",
        out_shape=[
            pltpu.VMEM((D_MODEL, WIDTH), bf16),
            pltpu.VMEM((D_MODEL, WIDTH), bf16),
            pltpu.VMEM((1, WIDTH), f32),
            pltpu.VMEM((1, WIDTH), f32),
            pltpu.VMEM((16, 128), bf16),
            pltpu.VMEM((ROWS, WIDTH), f32),
            pltpu.VMEM((ROWS, WIDTH), f32),
        ],
        in_specs=[anywhere] * 8,
        out_specs=[on_chip] * 7,
        scratch_shapes=[
            pltpu.VMEM((2 * ROWS, WIDTH), f32),
            pltpu.VMEM((2, ROWS, WIDTH), f32),
            pltpu.VMEM((2, 1, WIDTH), f32),
            pltpu.VMEM((24, 1, WIDTH), f32),
            pltpu.VMEM((16, 16, 128), f32),
            pltpu.VMEM((2, 1, 16), f32),
            pltpu.VMEM((RAW_TOTAL, WIDTH), f32),
            dma((5,)),
            dma,
            dma((len(GROUPS),)),
            dma,
            dma,
            dma,
            dma,
            dma((2,)),
            dma,
            dma((4,)),
        ],
        compiler_params=pltpu.CompilerParams(
            collective_id=0, has_side_effects=True, vmem_limit_bytes=30 * 1024 * 1024
        ),
    )(*(pltpu.with_memory_space_constraint(v, pltpu.HBM) for v in args))


def write_kernel(*refs):
    k = len(refs) // 2
    srcs, dsts, sem = refs[:k], refs[k : 2 * k], refs[2 * k]
    copies, count = [], 0
    for src, dst in zip(srcs, dsts):
        pieces = WRITE_PIECES if src.shape[0] == D_MODEL else 1
        rows = src.shape[0] // pieces
        for p in range(pieces):
            at = pl.ds(p * rows, rows)
            copies.append(pltpu.make_async_copy(src.at[at], dst.at[at], sem.at[count]))
            count += 1
    for copy in copies:
        copy.start()
    for copy in copies:
        copy.wait()


WRITE_PIECES = 4


def write(arrays):
    anywhere = pl.BlockSpec(memory_space=pl.ANY)
    return pl.pallas_call(
        write_kernel,
        name="write_kernel",
        out_shape=[jax.ShapeDtypeStruct(v.shape, v.dtype) for v in arrays],
        in_specs=[anywhere] * len(arrays),
        out_specs=[anywhere] * len(arrays),
        scratch_shapes=[pltpu.SemaphoreType.DMA((2 * WRITE_PIECES + 5,))],
        compiler_params=pltpu.CompilerParams(vmem_limit_bytes=1024 * 1024),
    )(*arrays)


def local(w_gate, first_gate, second_gate, w_up, first_up, second_up, norm_train, norm_step):
    norms = (norm_train.reshape(1, 16), norm_step.reshape(1, 16))
    held = gather(w_gate, first_gate, second_gate, w_up, first_up, second_up, *norms)
    ready_g, ready_u, col_g, col_u, norm, latest_g, latest_u = write(held)
    return (
        ready_g,
        ready_u,
        col_g.reshape(WIDTH),
        col_u.reshape(WIDTH),
        norm.reshape(D_MODEL),
        latest_g,
        latest_u,
    )


def solution(mesh):
    split = P("rows", "cols")
    return jax.shard_map(
        local,
        mesh=mesh,
        in_specs=(split,) * 6 + (P(("rows", "cols")),) * 2,
        out_specs=(P(None, "cols"),) * 2 + (P("cols"),) * 2 + (P(),) + (split,) * 2,
        check_vma=False,
    )
```

```python
import heapq

import jax
import jax.numpy as jnp
from jax import lax
from jax.experimental import pallas as pl
from jax.experimental.pallas import tpu as pltpu
from jax.sharding import PartitionSpec as P

D_MODEL = 2048
WIDTH = 2048
ROWS = 64
SIDE = 4
MESH = pl.DeviceIdType.MESH

learn_rate = 0.01
decay_rate = 0.1
tiny_value = 1e-08

CHUNKS = ((0, 0, 32), (1, 0, 16), (1, 16, 16), (0, 32, 32), (1, 32, 16), (1, 48, 16))
N = len(CHUNKS)
LOW = (0, 1, 2)
HIGH = (3, 4, 5)
FAR = (0, 1, 2, 0, 1, 2)
RAW_ROWS = 8
LINKS = ("A+", "A-", "B+", "B-")
NEIGHBOURS = {"A+": (3, 0), "A-": (1, 0), "B+": (0, 3), "B-": (0, 1)}
RAW = {0: LINKS, 1: ("A+", "A-")}
FINE_TAIL = 14


def follow_ups(da, db, c):
    if (da, db) == (0, 0):
        return tuple(k for k in LINKS if k not in RAW.get(c, ()))
    if db == 0:
        on = ("B+", "B-")
        if da == 3 and c in LOW:
            on = ("A+",) + on
        if da == 1 and c in HIGH:
            on = ("A-",) + on
        return on
    if db == 3 and c in LOW:
        return ("B+",)
    if db == 1 and c in HIGH:
        return ("B-",)
    return ()


def seen_by_receiver(link, da, db):
    step = -1 if link[1] == "+" else 1
    return ((da + step) % 4, db) if link[0] == "A" else (da, (db + step) % 4)


def arrival_order():
    delay = 1.4
    queues = {k: [] for k in LINKS}
    done = {k: 0.0 for k in queues}
    first = sorted([(0, 0, c) for c in range(N)], key=lambda v: len(RAW.get(v[2], ())) == 4)
    spot = len(first) - sum(len(k) == 4 for k in RAW.values())
    first[spot:spot] = [NEIGHBOURS[k] + (c,) for c in RAW for k in RAW[c]]
    events = [(0.0, i, item) for i, item in enumerate(first)]
    order, now, serial = [], 0.0, len(first)
    while events or any(queues.values()):
        rate = {}
        for k in queues:
            if queues[k]:
                other = ("B" if k[0] == "A" else "A") + k[1]
                size = CHUNKS[queues[k][0][2]][2] / 32
                rate[k] = (0.5 if queues[other] else 1.0) / size
        steps = [(1 - done[k]) / rate[k] for k in rate]
        if events:
            steps.append(events[0][0] - now)
        dt = max(0.0, min(steps))
        now += dt
        for k in rate:
            done[k] += rate[k] * dt
            if done[k] >= 1 - 1e-9:
                da, db, c = queues[k].pop(0)
                done[k] = 0.0
                serial += 1
                heapq.heappush(events, (now + delay, serial, seen_by_receiver(k, da, db) + (c,)))
        while events and events[0][0] <= now + 1e-9:
            item = heapq.heappop(events)[2]
            order.append(item)
            for k in follow_ups(*item):
                queues[k].append(item)
    return order


def group_of(da, db, c):
    if (da, db) in [NEIGHBOURS[k] for k in RAW.get(c, ())]:
        return ("raw", db == 0, c)
    if db == 0:
        return ("A", da % 2, c if da != 2 else FAR[c])
    return ("B", da, db % 2, c if db != 2 else FAR[c])


def die_copies(order):
    copies, waiting, seen = [], {}, {}
    last = {}
    for i, item in enumerate(order):
        last[item if item[:2] == (0, 0) else group_of(*item)] = i
    at = [(last[e if e[:2] == (0, 0) else group_of(*e)], e) for e in order]
    for i, (da, db, c) in sorted(at, key=lambda v: v[0]):
        mat, off, rows = CHUNKS[c]
        held = waiting.setdefault((da, db, mat), [])
        held.append((off, rows))
        seen[da, db, mat] = seen.get((da, db, mat), 0) + rows
        if i >= len(order) - FINE_TAIL:
            copies += [(i, da, db, mat, *piece) for piece in held]
            held.clear()
        elif seen[da, db, mat] == ROWS:
            copies.append((i, da, db, mat, 0, ROWS))
            held.clear()
    return copies


ORDER = arrival_order()
DIE = die_copies(ORDER)
SENT_ROWS = sum(len(follow_ups(*item)) * CHUNKS[item[2]][2] for item in ORDER)
RAW_TOTAL = sum(CHUNKS[c][2] * len(RAW[c]) for c in RAW)


GROUPS = {}
for _item in ORDER:
    if _item[:2] != (0, 0):
        GROUPS.setdefault(group_of(*_item), []).append(_item)
GROUP_NUMBER = {g: i for i, g in enumerate(GROUPS)}


def gather_kernel(
    w_g, f_g, s_g, w_u, f_u, s_u, n_t, n_s,
    out_g, out_u, col_g, col_u, norm_out, latest_g, latest_u,
    first, second, inverse, slots, nslots, n_in, raw,
    load_sem, send_sem, recv_sem, raw_send, die_send, die_recv,
    sum_send, sum_recv, n_send, n_recv,
):
    row = lax.axis_index("rows")
    x = lax.axis_index("cols")
    core = row % 2
    y = (row // 2) % 4
    z = row // 8
    a = y * core + z * (1 - core)
    b = z * core + y * (1 - core)
    stride_a = 8 - 6 * core
    stride_b = 2 + 6 * core
    partner = row + 1 - 2 * core
    outs = (out_g, out_u)
    latest = (latest_g, latest_u)

    def at_a(pos):
        return row + ((pos % 4) - a) * stride_a

    def at_b(pos):
        return row + ((pos % 4) - b) * stride_b

    def at_y(pos):
        return row + ((pos % 4) - y) * 2

    def at_z(pos):
        return row + ((pos % 4) - z) * 8

    places = ((y, z), (z, y))
    movers = ((at_y, at_z), (at_z, at_y))

    half = ROWS // 2

    def first_of(m):
        return first.at[pl.ds(m * ROWS, ROWS)]

    for m, (w, f, s) in enumerate(((w_g, f_g, s_g), (w_u, f_u, s_u))):
        for h in range(2):
            at = pl.ds(h * half, half)
            for src, dst in ((w, latest[m]), (f, first_of(m)), (s, second.at[m])):
                copy = pltpu.make_async_copy(
                    src.at[at], dst.at[at], load_sem.at[2 * m + h]
                )
                copy.start()
    for j, src in enumerate((n_t, n_s)):
        pltpu.make_async_copy(src, n_in.at[j], load_sem.at[4]).start()

    barrier = pltpu.get_barrier_semaphore()
    peers = [(partner, x)]
    for d in range(1, 4):
        peers += [(at_y(y + d), x), (at_z(z + d), x), (row, (x + d) % 4)]
        peers += [(at_y(y + d) + partner - row, x), (at_z(z + d) + partner - row, x)]
    for peer in peers:
        pl.semaphore_signal(barrier, inc=1, device_id=peer, device_id_type=MESH)

    for m in range(2):
        acc = jnp.zeros((8, WIDTH), jnp.float32)
        for h in range(2):
            three = first.at[pl.ds(0, 3 * half)]
            pltpu.make_async_copy(three, three, load_sem.at[2 * m + h]).wait()

            def step(i, acc, m=m):
                at = pl.ds(pl.multiple_of(i * 8, 8), 8)
                w = latest[m][at, :]
                new = w - learn_rate * (
                    first_of(m)[at, :] / (jnp.sqrt(second[m, at, :]) + tiny_value) + decay_rate * w
                )
                latest[m][at, :] = new
                return acc + jnp.abs(new)

            acc = lax.fori_loop(h * half // 8, (h + 1) * half // 8, step, acc, unroll=True)
        slots[8 * m + 2 * places[m][0] + core] = jnp.sum(acc, axis=0, keepdims=True)

    pl.semaphore_wait(barrier, len(peers))

    def remote(src, dst, send, recv, device):
        return pltpu.make_async_remote_copy(
            src_ref=src, dst_ref=dst, send_sem=send, recv_sem=recv,
            device_id=device, device_id_type=MESH,
        )

    def start(src, dst, send, recv, device):
        remote(src, dst, send, recv, device).start()

    def arrived(ref, recv):
        remote(ref, ref, send_sem, recv, (partner, x)).wait_recv()

    def left(ref, send):
        remote(ref, ref, send, die_recv, (partner, x)).wait_send()

    links = {
        "A+": (at_a(a + 1), x), "A-": (at_a(a + 3), x),
        "B+": (at_b(b + 1), x), "B-": (at_b(b + 3), x),
    }
    raw_pieces = [(c, p) for c in RAW for p in range(0, CHUNKS[c][2], RAW_ROWS)]

    raw_row, rows_so_far = {}, 0
    for c in RAW:
        for k in RAW[c]:
            raw_row[NEIGHBOURS[k] + (c,)] = rows_so_far
            rows_so_far += CHUNKS[c][2]

    def send_raw(number):
        for _ in range(number):
            if not raw_pieces:
                return
            c, p = raw_pieces.pop(0)
            mat, off, _ = CHUNKS[c]
            for k in RAW[c]:
                start(latest[mat].at[pl.ds(off + p, RAW_ROWS)],
                      raw.at[pl.ds(raw_row[NEIGHBOURS[k] + (c,)] + p, RAW_ROWS)], raw_send,
                      recv_sem.at[GROUP_NUMBER[group_of(*NEIGHBOURS[k], c)]], links[k])

    for d in (2, 1, 3, 0):
        for m in range(2):
            mine = slots.at[8 * m + 2 * places[m][0] + core]
            there = movers[m][0](places[m][0] + d)
            start(mine, mine, sum_send, sum_recv.at[0], (there + partner - row, x))
            if d:
                start(mine, mine, sum_send, sum_recv.at[0], (there, x))
    send_raw(RAW_BEFORE[0])

    def norm_stage(i, device_of, me):
        mine = nslots.at[4 * i + me]
        for d in range(1, 4):
            start(mine, mine, n_send, n_recv.at[i], device_of(d))

    def norm_wait(i):
        arrived(nslots.at[pl.ds(0, 3)], n_recv.at[i])
        total = nslots[4 * i]
        for k in range(1, 4):
            total = total + nslots[4 * i + k]
        return total

    pltpu.make_async_copy(n_in, n_in, load_sem.at[4]).wait()
    gain = n_in[0] + n_in[1]
    gain = jnp.broadcast_to(jnp.concatenate([gain] * 8, axis=1), (16, 128))
    place = lax.broadcasted_iota(jnp.int32, (16, 128), 0) * 8
    place = place + lax.broadcasted_iota(jnp.int32, (16, 128), 1) // 16
    nslots[x] = jnp.where(place == row * 4 + x, gain, 0.0)

    for stage, count in enumerate((8, 4)):
        if stage == 1:
            for d in (2, 1, 3):
                for m in range(2):
                    mine = slots.at[16 + 4 * m + places[m][1]]
                    start(mine, mine, sum_send, sum_recv.at[1],
                          (movers[m][1](places[m][1] + d), x))
            send_raw(RAW_BEFORE[1])
        arrived(slots.at[pl.ds(0, (14, 6)[stage])], sum_recv.at[stage])
        for m in range(2):
            terms = [slots[16 * stage + count * m + k] for k in range(count)]
            while len(terms) > 1:
                terms = [p + q for p, q in zip(terms[::2], terms[1::2])]
            if stage == 0:
                slots[16 + 4 * m + places[m][1]] = terms[0]
            else:
                column = terms[0] * (1.0 / D_MODEL)
                (col_g, col_u)[m][...] = column
                inverse[m] = 1.0 / column
    norm_stage(0, lambda d: (row, (x + d) % 4), x)

    def block_row(da, db):
        return row + ((a + da) % 4 - a) * stride_a + ((b + db) % 4 - b) * stride_b

    def rows_of(owner, mat, off, rows):
        return outs[mat].at[pl.ds(pl.multiple_of(owner * ROWS + off, 16), rows)]

    passed = [0]

    def pass_on(da, db, c):
        here = rows_of(block_row(da, db), *CHUNKS[c])
        for link in follow_ups(da, db, c):
            group = group_of(*seen_by_receiver(link, da, db), c)
            start(here, here, send_sem, recv_sem.at[GROUP_NUMBER[group]], links[link])

    def pass_over(i):
        while passed[0] < len(DIE) and DIE[passed[0]][0] == i:
            _, ea, eb, mat, off, rows = DIE[passed[0]]
            block = rows_of(block_row(ea, eb), mat, off, rows)
            start(block, block, die_send, die_recv, (partner, x))
            passed[0] += 1

    def scaled(value, mat):
        return (value * inverse[mat]).astype(jnp.bfloat16)

    def norm_step(s):
        if s == 3:
            arrived(nslots.at[13], n_recv.at[3])
            norm_out[...] = (nslots[12] + nslots[13]).astype(jnp.bfloat16)
            return
        total = norm_wait(s)
        if s == 0:
            nslots[4 + y] = total
            norm_stage(1, lambda d: (at_y(y + d), x), y)
        elif s == 1:
            nslots[8 + z] = total
            norm_stage(2, lambda d: (at_z(z + d), x), z)
        else:
            nslots[12] = total
            start(nslots.at[12], nslots.at[13], n_send, n_recv.at[3], (partner, x))

    waiting = {g: list(members) for g, members in GROUPS.items()}
    norm_at = [NORM_FIRST + NORM_EVERY * k for k in range(4)]
    for i, (da, db, c) in enumerate(ORDER):
        if i in norm_at:
            norm_step(norm_at.index(i))
        mat, off, rows = CHUNKS[c]
        if (da, db) == (0, 0):
            for p in range(0, rows, 16):
                at = pl.ds(pl.multiple_of(row * ROWS + off + p, 16), 16)
                outs[mat][at, :] = scaled(latest[mat][off + p : off + p + 16, :], mat)
            pass_on(da, db, c)
            pass_over(i)
            continue
        group = group_of(da, db, c)
        waiting[group].remove((da, db, c))
        if waiting[group]:
            continue
        total = sum(CHUNKS[e][2] for _, _, e in GROUPS[group])
        if group[0] == "raw":
            arrived(first.at[pl.ds(0, total)], recv_sem.at[GROUP_NUMBER[group]])
        else:
            arrived(outs[0].at[pl.ds(0, total)], recv_sem.at[GROUP_NUMBER[group]])
        for ea, eb, e in GROUPS[group]:
            mat, off, rows = CHUNKS[e]
            if group[0] == "raw":
                for p in range(0, rows, 16):
                    at = pl.ds(pl.multiple_of(block_row(ea, eb) * ROWS + off + p, 16), 16)
                    r = raw_row[ea, eb, e] + p
                    outs[mat][at, :] = scaled(raw[r : r + 16, :], mat)
            pass_on(ea, eb, e)
        pass_over(i)

    arrived(outs[0], die_recv)
    left(outs[0], die_send)
    left(outs[0].at[pl.ds(0, SENT_ROWS)], send_sem)
    left(raw, raw_send)
    left(slots.at[pl.ds(0, 20)], sum_send)
    left(nslots.at[pl.ds(0, 10)], n_send)


NORM_FIRST, NORM_EVERY = 12, 10
RAW_BEFORE = (3, 3)


def gather(*args):
    f32, bf16 = jnp.float32, jnp.bfloat16
    dma = pltpu.SemaphoreType.DMA
    anywhere = pl.BlockSpec(memory_space=pl.ANY)
    on_chip = pl.BlockSpec(memory_space=pltpu.VMEM)
    return pl.pallas_call(
        gather_kernel,
        name="gather_kernel",
        out_shape=[
            pltpu.VMEM((D_MODEL, WIDTH), bf16),
            pltpu.VMEM((D_MODEL, WIDTH), bf16),
            pltpu.VMEM((1, WIDTH), f32),
            pltpu.VMEM((1, WIDTH), f32),
            pltpu.VMEM((16, 128), bf16),
            pltpu.VMEM((ROWS, WIDTH), f32),
            pltpu.VMEM((ROWS, WIDTH), f32),
        ],
        in_specs=[anywhere] * 8,
        out_specs=[on_chip] * 7,
        scratch_shapes=[
            pltpu.VMEM((2 * ROWS, WIDTH), f32),
            pltpu.VMEM((2, ROWS, WIDTH), f32),
            pltpu.VMEM((2, 1, WIDTH), f32),
            pltpu.VMEM((24, 1, WIDTH), f32),
            pltpu.VMEM((16, 16, 128), f32),
            pltpu.VMEM((2, 1, 16), f32),
            pltpu.VMEM((RAW_TOTAL, WIDTH), f32),
            dma((5,)),
            dma,
            dma((len(GROUPS),)),
            dma,
            dma,
            dma,
            dma,
            dma((2,)),
            dma,
            dma((4,)),
        ],
        compiler_params=pltpu.CompilerParams(
            collective_id=0, has_side_effects=True, vmem_limit_bytes=30 * 1024 * 1024
        ),
    )(*(pltpu.with_memory_space_constraint(v, pltpu.HBM) for v in args))


def write_kernel(*refs):
    k = len(refs) // 2
    srcs, dsts, sem = refs[:k], refs[k : 2 * k], refs[2 * k]
    copies, count = [], 0
    for src, dst in zip(srcs, dsts):
        pieces = WRITE_PIECES if src.shape[0] == D_MODEL else 1
        rows = src.shape[0] // pieces
        for p in range(pieces):
            at = pl.ds(p * rows, rows)
            copies.append(pltpu.make_async_copy(src.at[at], dst.at[at], sem.at[count]))
            count += 1
    for copy in copies:
        copy.start()
    for copy in copies:
        copy.wait()


WRITE_PIECES = 2


def write(arrays):
    anywhere = pl.BlockSpec(memory_space=pl.ANY)
    return pl.pallas_call(
        write_kernel,
        name="write_kernel",
        out_shape=[jax.ShapeDtypeStruct(v.shape, v.dtype) for v in arrays],
        in_specs=[anywhere] * len(arrays),
        out_specs=[anywhere] * len(arrays),
        scratch_shapes=[pltpu.SemaphoreType.DMA((2 * WRITE_PIECES + 5,))],
        compiler_params=pltpu.CompilerParams(vmem_limit_bytes=1024 * 1024),
    )(*arrays)


def local(w_gate, first_gate, second_gate, w_up, first_up, second_up, norm_train, norm_step):
    norms = (norm_train.reshape(1, 16), norm_step.reshape(1, 16))
    held = gather(w_gate, first_gate, second_gate, w_up, first_up, second_up, *norms)
    ready_g, ready_u, col_g, col_u, norm, latest_g, latest_u = write(held)
    return (
        ready_g,
        ready_u,
        col_g.reshape(WIDTH),
        col_u.reshape(WIDTH),
        norm.reshape(D_MODEL),
        latest_g,
        latest_u,
    )


def solution(mesh):
    split = P("rows", "cols")
    return jax.shard_map(
        local,
        mesh=mesh,
        in_specs=(split,) * 6 + (P(("rows", "cols")),) * 2,
        out_specs=(P(None, "cols"),) * 2 + (P("cols"),) * 2 + (P(),) + (split,) * 2,
        check_vma=False,
    )
```
